64 devices in a mesh: dp: 4 (over x, y), sp: 16 (over z, core).
Axes of the slice: x: 2, y: 2, z: 8, core: 2. Of those that a mesh axis runs over, the one named last changes fastest.
The devices are a block of a 4x4x8 slice.
Arguments:
- x: bfloat16 [32, 2048, 128], P('dp', 'sp'), parts along dimension 0
- w_cur: bfloat16 [16, 10, 128, 256], replicated
- w_past: bfloat16 [16, 10, 128, 256], replicated
- w_res: bfloat16 [16, 10, 128, 128], replicated
- w_skip: bfloat16 [16, 10, 128, 128], replicated
Outputs:
- output 1: float32 [32, 16, 128, 128], P('dp', 'sp'), parts along dimension 0
- output 2: float32 [32, 16, 128, 128], P('dp', 'sp'), parts along dimension 0
There are 4 independent parts. The reference program is written for one: setup_inputs(seed, part) draws one part's arguments, and reference() takes and returns one part's arrays. A program takes and returns all parts, laid end to end along the dimension named above; an argument that names none is the same for every part.
All inputs are finite; a program needn't handle non-finite values.
Results may differ from the reference program's by a relative error of at most 0.00880401.
Values are sent between devices in bfloat16 or wider.
A program may use at most 768 MiB of HBM per device.

```python
import jax
import jax.numpy as jnp
from jax import lax

BATCH_PART = 8
SEQ_DEV = 128
GROUP_SIZE = 16
STACKS = 16
CHANNELS = 128
SKIP_CH = 128
CYCLE_LEN = 10

SEQ_LEN = SEQ_DEV * GROUP_SIZE
LAYERS = STACKS * CYCLE_LEN


def setup_inputs(seed: int = 0, part: int = 0) -> dict:
    base_key = jax.random.key(seed)
    key_x = jax.random.fold_in(jax.random.fold_in(base_key, 1), part)
    key_w = jax.random.split(jax.random.fold_in(base_key, 2), 4)
    tap_scale = (2 * CHANNELS) ** -0.5
    out_scale = 2.0 * (CHANNELS * LAYERS) ** -0.5
    tap_shape = (STACKS, CYCLE_LEN, CHANNELS, 2 * CHANNELS)
    x = jax.random.normal(key_x, (BATCH_PART, SEQ_LEN, CHANNELS), jnp.float32)
    w_cur = jax.random.normal(key_w[0], tap_shape, jnp.float32) * tap_scale
    w_past = jax.random.normal(key_w[1], tap_shape, jnp.float32) * tap_scale
    w_res = jax.random.normal(key_w[2], (STACKS, CYCLE_LEN, CHANNELS, CHANNELS), jnp.float32) * out_scale
    w_skip = jax.random.normal(key_w[3], (STACKS, CYCLE_LEN, CHANNELS, SKIP_CH), jnp.float32) * out_scale
    return {"x": x.astype(jnp.bfloat16), "w_cur": w_cur.astype(jnp.bfloat16), "w_past": w_past.astype(jnp.bfloat16), "w_res": w_res.astype(jnp.bfloat16), "w_skip": w_skip.astype(jnp.bfloat16)}


def gated_layer(h_res, skip_acc, cur_w, past_w, res_w, skip_w, dilation):
    row_count = BATCH_PART * SEQ_LEN
    u_cur = h_res.astype(jnp.bfloat16)
    u_past = jnp.concatenate([jnp.zeros((BATCH_PART, dilation, CHANNELS), jnp.bfloat16), u_cur[:, :SEQ_LEN - dilation]], axis=1)
    pre_act = jnp.dot(u_cur.reshape(row_count, CHANNELS), cur_w, preferred_element_type=jnp.float32) + jnp.dot(u_past.reshape(row_count, CHANNELS), past_w, preferred_element_type=jnp.float32)
    gated = (jnp.tanh(pre_act[:, :CHANNELS]) * jax.nn.sigmoid(pre_act[:, CHANNELS:])).astype(jnp.bfloat16)
    h_new = h_res + jnp.dot(gated, res_w, preferred_element_type=jnp.float32).reshape(BATCH_PART, SEQ_LEN, CHANNELS)
    skip_new = skip_acc + jnp.dot(gated, skip_w, preferred_element_type=jnp.float32).reshape(BATCH_PART, SEQ_LEN, SKIP_CH)
    return h_new, skip_new


def reference(x, w_cur, w_past, w_res, w_skip):
    def stack_body(carry, weights):
        h_res, skip_acc = carry
        stack_cur, stack_past, stack_res, stack_skip = weights
        for layer_pos in range(CYCLE_LEN):
            h_res, skip_acc = gated_layer(h_res, skip_acc, stack_cur[layer_pos], stack_past[layer_pos], stack_res[layer_pos], stack_skip[layer_pos], 2 ** layer_pos)
        return (h_res, skip_acc), None

    h_start = x.astype(jnp.float32)
    skip_start = jnp.zeros((BATCH_PART, SEQ_LEN, SKIP_CH), jnp.float32)
    (h_fin, skip_fin), unused = lax.scan(stack_body, (h_start, skip_start), (w_cur, w_past, w_res, w_skip))
    h_out = h_fin.reshape(BATCH_PART, SEQ_DEV, GROUP_SIZE, CHANNELS).transpose(0, 2, 1, 3)
    skip_out = skip_fin.reshape(BATCH_PART, SEQ_DEV, GROUP_SIZE, SKIP_CH).transpose(0, 2, 1, 3)
    return (h_out, skip_out)
```

```python
import functools

import jax
import jax.numpy as jnp
from jax import lax
from jax.experimental import pallas as pl
from jax.experimental.pallas import tpu as pltpu
from jax.sharding import PartitionSpec as P

F32, BF16 = jnp.float32, jnp.bfloat16
BLOCK = 256
LAG_GATE, LAG_ADD = 2, 4
GROUP = 2


def halo_slots(cycle_len):
    sizes = [max(16, 2**layer) for layer in range(cycle_len)]
    starts = [sum(sizes[:layer]) for layer in range(cycle_len)]
    return sizes, starts, sum(sizes)


def kernel(group_n, x_hbm, wc_hbm, wp_hbm, wr_hbm, ws_hbm, h_out, s_out, w_cur, w_past, w_res, w_skip, h_buf, s_buf, u_buf, halo, tail, x_in, x_all,
           h_stage, s_stage, w_sem, x_sem, x_send, x_recv, halo_send, halo_recv, out_send, out_recv):
    batch_n, seq_dev, chan = x_in.shape
    stacks, cycle_len = w_cur.shape[:2]
    rows = batch_n * seq_dev
    cores = group_n // batch_n
    pad = u_buf.shape[1] - rows
    top = h_buf.shape[0] - rows
    sizes, starts, halo_rows = halo_slots(cycle_len)
    me = lax.axis_index("sp")
    chip, core = me // cores, lax.rem(me, cores)
    far_first = sorted(range(batch_n), key=lambda off: -min(off, batch_n - off))

    x_copy = pltpu.make_async_copy(x_hbm, x_in, x_sem)
    x_copy.start()
    pairs = ((wc_hbm, w_cur), (wp_hbm, w_past), (wr_hbm, w_res), (ws_hbm, w_skip))

    def weight_copies(turn):
        part = pl.ds(turn * GROUP, GROUP)
        return [pltpu.make_async_copy(src.at[part], dst.at[part], w_sem.at[turn, k]) for k, (src, dst) in enumerate(pairs)]

    for turn in range(stacks // GROUP):
        for copy in weight_copies(turn):
            copy.start()

    barrier = pltpu.get_barrier_semaphore()
    for off in range(1, group_n):
        pl.semaphore_signal(barrier, inc=1, device_id={"sp": lax.rem(me + off, group_n)}, device_id_type=pl.DeviceIdType.MESH)

    @pl.when(core == 0)
    def _():
        halo[...] = jnp.zeros_like(halo)

    s_buf[...] = jnp.zeros_like(s_buf)
    h_buf[0:top, :] = jnp.zeros((top, chan), F32)
    pl.semaphore_wait(barrier, group_n - 1)

    half, place = me // batch_n, lax.rem(me, batch_n)
    x_copy.wait()

    def x_copies(off):
        seq = lax.rem(chip + off, batch_n)
        target = seq * cores + half
        dst = x_all.at[pl.ds(place * seq_dev, seq_dev)]

        def local():
            return pltpu.make_async_copy(x_in.at[seq], dst, x_recv.at[place])

        def remote():
            return pltpu.make_async_remote_copy(x_in.at[seq], dst, x_send.at[off], x_recv.at[place], device_id={"sp": target},
                                                device_id_type=pl.DeviceIdType.MESH)

        return target, local, remote

    for off in far_first:
        target, local, remote = x_copies(off)
        if off:
            remote().start()
        else:
            pl.when(target == me)(lambda: local().start())
            pl.when(target != me)(lambda: remote().start())
    for src in range(batch_n):
        dst = x_all.at[pl.ds(src * seq_dev, seq_dev)]
        pltpu.make_async_copy(dst, dst, x_recv.at[src]).wait()
    x = x_all[...]
    h_buf[top:, :] = x.astype(F32)
    u_buf[0, pad:, :] = x
    tail[0, starts[0]:starts[0] + sizes[0], :] = x[rows - sizes[0]:]

    def halo_copy(turn):
        part = pl.ds(turn * GROUP, GROUP)
        return pltpu.make_async_remote_copy(tail.at[part], halo.at[part], halo_send.at[turn], halo_recv.at[turn],
                                            device_id={"sp": jnp.minimum(me + 1, group_n - 1)}, device_id_type=pl.DeviceIdType.MESH)

    blocks = rows // BLOCK

    def dot(lhs, rhs):
        return jnp.dot(lhs, rhs, preferred_element_type=F32)

    def group_of_stacks(turn, carry):
        base = turn * GROUP
        for copy in weight_copies(turn):
            copy.wait()
        pl.when(core > 0)(lambda: halo_copy(turn).wait_recv())
        pre, outs = {}, {}

        def taps(step):
            layer, block = divmod(step, blocks)
            part, pos = divmod(layer, cycle_len)
            dilation = 2**pos
            if block == 0:
                got = halo[base + part, starts[pos]:starts[pos] + sizes[pos], :]
                u_buf[pos, pad - sizes[pos]:pad, :] = got
                if pos == 0:
                    h_buf[0:top, :] = got[sizes[pos] - top:].astype(F32)
            at = pad + block * BLOCK
            now = u_buf[pos, at:at + BLOCK, :]
            if dilation == 1:
                past = h_buf[top + block * BLOCK - 1:top + (block + 1) * BLOCK - 1, :].astype(BF16)
            else:
                past = u_buf[pos, at - dilation:at - dilation + BLOCK, :]
            both = jnp.concatenate([w_cur[base + part, pos], w_past[base + part, pos]], axis=0)
            pre[step] = dot(jnp.concatenate([now, past], axis=1), both)

        def gate(step):
            part, pos = divmod(step // blocks, cycle_len)
            z = pre.pop(step)
            a = (jnp.tanh(z[:, :chan]) * (0.5 * jnp.tanh(0.5 * z[:, chan:]) + 0.5)).astype(BF16)
            outs[step] = dot(a, jnp.concatenate([w_res[base + part, pos], w_skip[base + part, pos]], axis=1))

        def add(step):
            layer, block = divmod(step, blocks)
            part, pos = divmod(layer + 1, cycle_len)
            out = outs.pop(step)
            first, last = block * BLOCK, (block + 1) * BLOCK
            h = h_buf[top + first:top + last, :] + out[:, :chan]
            h_buf[top + first:top + last, :] = h
            s_buf[first:last, :] = s_buf[first:last, :] + out[:, chan:]
            u = h.astype(BF16)
            u_buf[pos, pad + first:pad + last, :] = u
            kept = max(first, rows - sizes[pos])
            if kept < last:
                at = starts[pos] + kept - (rows - sizes[pos])
                tail[base + part, at:at + last - kept, :] = u[kept - first:]

        steps = GROUP * cycle_len * blocks
        for step in range(steps + LAG_ADD):
            if step >= LAG_ADD:
                add(step - LAG_ADD)
            if LAG_GATE <= step < steps + LAG_GATE:
                gate(step - LAG_GATE)
            if step < steps:
                taps(step)
        pl.when(core < cores - 1)(lambda: halo_copy(turn).start())
        return carry

    lax.fori_loop(0, stacks // GROUP, group_of_stacks, 0)

    part_rows = rows // group_n
    spread = [(off, sub) for off in far_first for sub in range(cores)]

    def out_target(off, sub):
        return lax.rem(chip + off, batch_n) * cores + sub

    def out_copies(off, sub):
        target = out_target(off, sub)
        rank = off * cores + sub
        found = []
        for kind, (stage, out) in enumerate(((s_stage, s_out), (h_stage, h_out))):
            dst = out.at[chip, 0, pl.ds(core * part_rows, part_rows)]

            def local(kind=kind, stage=stage, dst=dst):
                return pltpu.make_async_copy(stage.at[target], dst, out_recv.at[kind, me])

            def remote(kind=kind, stage=stage, dst=dst):
                return pltpu.make_async_remote_copy(stage.at[target], dst, out_send.at[kind, rank], out_recv.at[kind, me],
                                                    device_id={"sp": target}, device_id_type=pl.DeviceIdType.MESH)

            found.append((local, remote))
        return target, found

    def send(off, sub):
        target, found = out_copies(off, sub)
        for local, remote in found:
            if off:
                remote().start()
            else:
                pl.when(target == me)(lambda: local().start())
                pl.when(target != me)(lambda: remote().start())

    for rank, (off, sub) in enumerate(spread):
        target = out_target(off, sub)
        s_stage[target] = s_buf[pl.ds(target, part_rows, stride=group_n), :]
        h_stage[target] = h_buf[pl.ds(top + target, part_rows, stride=group_n), :]
        if rank:
            send(*spread[rank - 1])
    send(*spread[-1])

    for off in range(batch_n):
        target, local, remote = x_copies(off)
        if off:
            remote().wait_send()
        else:
            pl.when(target != me)(lambda: remote().wait_send())

    def end_halo(turn, carry):
        halo_copy(turn).wait_send()
        return carry

    @pl.when(core < cores - 1)
    def _():
        lax.fori_loop(0, stacks // GROUP, end_halo, 0)

    for off, sub in spread:
        target, found = out_copies(off, sub)
        for local, remote in found:
            if off:
                remote().wait_send()
            else:
                pl.when(target != me)(lambda: remote().wait_send())
    for src in range(group_n):
        for kind, out in enumerate((s_out, h_out)):
            dst = out.at[src // cores, 0, pl.ds(src % cores * part_rows, part_rows)]
            pltpu.make_async_copy(dst, dst, out_recv.at[kind, src]).wait()


def solution(mesh):
    group_n = mesh.shape["sp"]

    def local_stack(x, w_cur, w_past, w_res, w_skip):
        batch_n, seq_dev, chan = x.shape
        stacks, cycle_len = w_cur.shape[:2]
        rows = batch_n * seq_dev
        sizes, starts, halo_rows = halo_slots(cycle_len)
        pad, top = 2 ** (cycle_len - 1), 8
        turns = stacks // GROUP
        vmem, dma = pltpu.VMEM, pltpu.SemaphoreType.DMA
        out = jax.ShapeDtypeStruct((batch_n, 1, seq_dev, chan), F32)
        hbm = pl.BlockSpec(memory_space=pltpu.HBM)
        return pl.pallas_call(
            functools.partial(kernel, group_n),
            out_shape=[out, out],
            in_specs=[hbm] * 5,
            out_specs=[hbm] * 2,
            scratch_shapes=[
                vmem(w_cur.shape, BF16), vmem(w_past.shape, BF16), vmem(w_res.shape, BF16), vmem(w_skip.shape, BF16),
                vmem((top + rows, chan), F32), vmem((rows, chan), F32), vmem((cycle_len, pad + rows, chan), BF16),
                vmem((stacks, halo_rows, chan), BF16), vmem((stacks + 1, halo_rows, chan), BF16),
                vmem(x.shape, BF16), vmem((rows, chan), BF16),
                vmem((group_n, rows // group_n, chan), F32), vmem((group_n, rows // group_n, chan), F32),
                dma((turns, 4)), dma, dma((batch_n,)), dma((batch_n,)), dma((turns,)), dma((turns,)), dma((2, group_n)), dma((2, group_n)),
            ],
            compiler_params=pltpu.CompilerParams(collective_id=0, has_side_effects=True, vmem_limit_bytes=60 * 2**20),
        )(x, w_cur, w_past, w_res, w_skip)

    return jax.shard_map(local_stack, mesh=mesh, in_specs=(P("dp", "sp", None), P(), P(), P(), P()),
                         out_specs=(P("dp", "sp", None, None), P("dp", "sp", None, None)), check_vma=False)
```

```python
import functools

import jax
import jax.numpy as jnp
from jax import lax
from jax.experimental import pallas as pl
from jax.experimental.pallas import tpu as pltpu
from jax.sharding import PartitionSpec as P

F32, BF16 = jnp.float32, jnp.bfloat16
BLOCK = 512
LAG = 1
GROUP = 2


def halo_slots(cycle_len):
    sizes = [max(16, 2**layer) for layer in range(cycle_len)]
    starts = [sum(sizes[:layer]) for layer in range(cycle_len)]
    return sizes, starts, sum(sizes)


def kernel(group_n, x_hbm, wc_hbm, wp_hbm, wr_hbm, ws_hbm, both_out, w_cur, w_past, w_res, w_skip, h_buf, s_buf, u_buf, halo, tail, x_in, x_all,
           stage, w_sem, x_sem, x_send, x_recv, halo_send, halo_recv, out_send, out_recv):
    batch_n, seq_dev, chan = x_in.shape
    stacks, cycle_len = w_cur.shape[:2]
    rows = batch_n * seq_dev
    cores = group_n // batch_n
    pad = u_buf.shape[1] - rows
    top = h_buf.shape[0] - rows
    sizes, starts, halo_rows = halo_slots(cycle_len)
    me = lax.axis_index("sp")
    chip, core = me // cores, lax.rem(me, cores)
    far_first = sorted(range(batch_n), key=lambda off: -min(off, batch_n - off))

    x_copy = pltpu.make_async_copy(x_hbm, x_in, x_sem)
    x_copy.start()
    pairs = ((wc_hbm, w_cur), (wp_hbm, w_past), (wr_hbm, w_res), (ws_hbm, w_skip))

    def weight_copies(turn):
        part = pl.ds(turn * GROUP, GROUP)
        return [pltpu.make_async_copy(src.at[part], dst.at[part], w_sem.at[turn, k]) for k, (src, dst) in enumerate(pairs)]

    for turn in range(stacks // GROUP):
        for copy in weight_copies(turn):
            copy.start(priority=1)

    barrier = pltpu.get_barrier_semaphore()
    for off in range(1, group_n):
        pl.semaphore_signal(barrier, inc=1, device_id={"sp": lax.rem(me + off, group_n)}, device_id_type=pl.DeviceIdType.MESH)

    @pl.when(core == 0)
    def _():
        halo[...] = jnp.zeros_like(halo)

    s_buf[...] = jnp.zeros_like(s_buf)
    h_buf[0:top, :] = jnp.zeros((top, chan), F32)
    pl.semaphore_wait(barrier, group_n - 1)

    half, place = me // batch_n, lax.rem(me, batch_n)
    x_copy.wait()

    def x_copies(off):
        seq = lax.rem(chip + off, batch_n)
        target = seq * cores + half
        dst = x_all.at[pl.ds(place * seq_dev, seq_dev)]

        def local():
            return pltpu.make_async_copy(x_in.at[seq], dst, x_recv.at[place])

        def remote():
            return pltpu.make_async_remote_copy(x_in.at[seq], dst, x_send.at[off], x_recv.at[place], device_id={"sp": target},
                                                device_id_type=pl.DeviceIdType.MESH)

        return target, local, remote

    for off in far_first:
        target, local, remote = x_copies(off)
        if off:
            remote().start()
        else:
            pl.when(target == me)(lambda: local().start())
            pl.when(target != me)(lambda: remote().start())
    for src in range(batch_n):
        dst = x_all.at[pl.ds(src * seq_dev, seq_dev)]
        pltpu.make_async_copy(dst, dst, x_recv.at[src]).wait()
    x = x_all[...]
    h_buf[top:, :] = x.astype(F32)
    u_buf[0, pad:, :] = x
    tail[0, starts[0]:starts[0] + sizes[0], :] = x[rows - sizes[0]:]

    def halo_copy(turn):
        part = pl.ds(turn * GROUP, GROUP)
        return pltpu.make_async_remote_copy(tail.at[part], halo.at[part], halo_send.at[turn], halo_recv.at[turn],
                                            device_id={"sp": jnp.minimum(me + 1, group_n - 1)}, device_id_type=pl.DeviceIdType.MESH)

    blocks = rows // BLOCK

    def dot(lhs, rhs):
        return jnp.dot(lhs, rhs, preferred_element_type=F32)

    def group_of_stacks(turn, carry):
        base = turn * GROUP
        for copy in weight_copies(turn):
            copy.wait()
        pl.when(core > 0)(lambda: halo_copy(turn).wait_recv())
        pre, outs = {}, {}

        def taps(step):
            layer, block = divmod(step, blocks)
            part, pos = divmod(layer, cycle_len)
            dilation = 2**pos
            if block == 0:
                got = halo[base + part, starts[pos]:starts[pos] + sizes[pos], :]
                u_buf[pos, pad - sizes[pos]:pad, :] = got
                if pos == 0:
                    h_buf[0:top, :] = got[sizes[pos] - top:].astype(F32)
            at = pad + block * BLOCK
            now = u_buf[pos, at:at + BLOCK, :]
            if dilation == 1:
                past = h_buf[top + block * BLOCK - 1:top + (block + 1) * BLOCK - 1, :].astype(BF16)
            else:
                past = u_buf[pos, at - dilation:at - dilation + BLOCK, :]
            both = jnp.concatenate([w_cur[base + part, pos], w_past[base + part, pos]], axis=0)
            pre[step] = dot(jnp.concatenate([now, past], axis=1), both)

        def gate(step):
            part, pos = divmod(step // blocks, cycle_len)
            z = pre.pop(step)
            a = (jnp.tanh(z[:, :chan]) * (0.5 * jnp.tanh(0.5 * z[:, chan:]) + 0.5)).astype(BF16)
            outs[step] = dot(a, jnp.concatenate([w_res[base + part, pos], w_skip[base + part, pos]], axis=1))

        def add(step):
            layer, block = divmod(step, blocks)
            part, pos = divmod(layer + 1, cycle_len)
            out = outs.pop(step)
            first, last = block * BLOCK, (block + 1) * BLOCK
            h = h_buf[top + first:top + last, :] + out[:, :chan]
            h_buf[top + first:top + last, :] = h
            s_buf[first:last, :] = s_buf[first:last, :] + out[:, chan:]
            u = h.astype(BF16)
            u_buf[pos, pad + first:pad + last, :] = u
            kept = max(first, rows - sizes[pos])
            if kept < last:
                at = starts[pos] + kept - (rows - sizes[pos])
                tail[base + part, at:at + last - kept, :] = u[kept - first:]

        steps = GROUP * cycle_len * blocks
        for step in range(steps + LAG):
            if step < steps:
                taps(step)
            if step >= LAG:
                gate(step - LAG)
                add(step - LAG)
        pl.when(core < cores - 1)(lambda: halo_copy(turn).start())
        return carry

    lax.fori_loop(0, stacks // GROUP, group_of_stacks, 0)

    part_rows = rows // group_n
    spread = [(off, sub) for off in far_first for sub in range(cores)]

    def out_target(off, sub):
        return lax.rem(chip + off, batch_n) * cores + sub

    def out_copies(off, sub):
        target = out_target(off, sub)
        dst = both_out.at[:, chip, core]

        def remote():
            return pltpu.make_async_remote_copy(stage.at[target], dst, out_send.at[off * cores + sub], out_recv.at[me],
                                                device_id={"sp": target}, device_id_type=pl.DeviceIdType.MESH)

        return target, remote

    def send(off, sub):
        target, remote = out_copies(off, sub)
        if off:
            remote().start()
        else:
            @pl.when(target == me)
            def _():
                both_out[:, chip, core] = stage[target]

            pl.when(target != me)(lambda: remote().start())

    for rank, (off, sub) in enumerate(spread):
        target = out_target(off, sub)
        stage[target, 1] = s_buf[pl.ds(target, part_rows, stride=group_n), :]
        stage[target, 0] = h_buf[pl.ds(top + target, part_rows, stride=group_n), :]
        if rank:
            send(*spread[rank - 1])
    send(*spread[-1])

    for off in range(batch_n):
        target, local, remote = x_copies(off)
        if off:
            remote().wait_send()
        else:
            pl.when(target != me)(lambda: remote().wait_send())

    def end_halo(turn, carry):
        halo_copy(turn).wait_send()
        return carry

    @pl.when(core < cores - 1)
    def _():
        lax.fori_loop(0, stacks // GROUP, end_halo, 0)

    for off, sub in spread:
        target, remote = out_copies(off, sub)
        if off:
            remote().wait_send()
        else:
            pl.when(target != me)(lambda: remote().wait_send())
    for src in range(group_n):
        dst = both_out.at[:, src // cores, src % cores]

        @pl.when(src != me)
        def _():
            pltpu.make_async_copy(dst, dst, out_recv.at[src]).wait()


def write_out(both, h_out, s_out, sems):
    copies = [pltpu.make_async_copy(both.at[kind], out, sems.at[kind]) for kind, out in enumerate((h_out, s_out))]
    for copy in copies:
        copy.start()
    for copy in copies:
        copy.wait()


def solution(mesh):
    group_n = mesh.shape["sp"]

    def local_stack(x, w_cur, w_past, w_res, w_skip):
        batch_n, seq_dev, chan = x.shape
        stacks, cycle_len = w_cur.shape[:2]
        rows = batch_n * seq_dev
        sizes, starts, halo_rows = halo_slots(cycle_len)
        pad, top = 2 ** (cycle_len - 1), 8
        turns = stacks // GROUP
        vmem, dma = pltpu.VMEM, pltpu.SemaphoreType.DMA
        cores, part_rows = group_n // batch_n, rows // group_n
        hbm, in_vmem = pl.BlockSpec(memory_space=pltpu.HBM), pl.BlockSpec(memory_space=vmem)
        both = pl.pallas_call(
            functools.partial(kernel, group_n),
            out_shape=vmem((2, batch_n, cores, part_rows, chan), F32),
            in_specs=[hbm] * 5,
            out_specs=in_vmem,
            scratch_shapes=[
                vmem(w_cur.shape, BF16), vmem(w_past.shape, BF16), vmem(w_res.shape, BF16), vmem(w_skip.shape, BF16),
                vmem((top + rows, chan), F32), vmem((rows, chan), F32), vmem((cycle_len, pad + rows, chan), BF16),
                vmem((stacks, halo_rows, chan), BF16), vmem((stacks + 1, halo_rows, chan), BF16),
                vmem(x.shape, BF16), vmem((rows, chan), BF16),
                vmem((group_n, 2, part_rows, chan), F32),
                dma((turns, 4)), dma, dma((batch_n,)), dma((batch_n,)), dma((turns,)), dma((turns,)), dma((group_n,)), dma((group_n,)),
            ],
            compiler_params=pltpu.CompilerParams(collective_id=0, has_side_effects=True, vmem_limit_bytes=50 * 2**20),
        )(pltpu.with_memory_space_constraint(x, pltpu.HBM), w_cur, w_past, w_res, w_skip)
        both = pltpu.with_memory_space_constraint(both, pltpu.VMEM)
        out = jax.ShapeDtypeStruct((batch_n, cores, part_rows, chan), F32)
        outs = pl.pallas_call(write_out, out_shape=[out, out], in_specs=[in_vmem], out_specs=[hbm] * 2, scratch_shapes=[dma((2,))])(both)
        return tuple(o.reshape(batch_n, 1, seq_dev, chan) for o in outs)

    return jax.shard_map(local_stack, mesh=mesh, in_specs=(P("dp", "sp", None), P(), P(), P(), P()),
                         out_specs=(P("dp", "sp", None, None), P("dp", "sp", None, None)), check_vma=False)
```

```python
import functools

import jax
import jax.numpy as jnp
from jax import lax
from jax.experimental import pallas as pl
from jax.experimental.pallas import tpu as pltpu
from jax.sharding import PartitionSpec as P

F32, BF16 = jnp.float32, jnp.bfloat16
GROUP = 2


def halo_slots(cycle_len):
    sizes = [max(16, 2**layer) for layer in range(cycle_len)]
    starts = [sum(sizes[:layer]) for layer in range(cycle_len)]
    return sizes, starts, sum(sizes)


def kernel(group_n, x_hbm, wc_hbm, wp_hbm, wr_hbm, ws_hbm, both_out, w_cur, w_past, w_res, w_skip, h_buf, s_buf, u_buf, halo, tail, x_in, x_all,
           stage, w_sem, x_sem, x_send, x_recv, halo_send, halo_recv, out_send, out_recv):
    batch_n, seq_dev, chan = x_in.shape
    stacks, cycle_len = w_cur.shape[:2]
    rows = batch_n * seq_dev
    cores = group_n // batch_n
    pad = u_buf.shape[1] - rows
    top = h_buf.shape[0] - rows
    sizes, starts, halo_rows = halo_slots(cycle_len)
    me = lax.axis_index("sp")
    chip, core = me // cores, lax.rem(me, cores)
    far_first = sorted(range(batch_n), key=lambda off: -min(off, batch_n - off))

    x_copy = pltpu.make_async_copy(x_hbm, x_in, x_sem)
    x_copy.start()
    pairs = ((wc_hbm, w_cur), (wp_hbm, w_past), (wr_hbm, w_res), (ws_hbm, w_skip))

    def weight_copies(turn):
        part = pl.ds(turn * GROUP, GROUP)
        return [pltpu.make_async_copy(src.at[part], dst.at[part], w_sem.at[turn, k]) for k, (src, dst) in enumerate(pairs)]

    for turn in range(stacks // GROUP):
        for copy in weight_copies(turn):
            copy.start(priority=1)

    barrier = pltpu.get_barrier_semaphore()
    for off in range(1, group_n):
        pl.semaphore_signal(barrier, inc=1, device_id={"sp": lax.rem(me + off, group_n)}, device_id_type=pl.DeviceIdType.MESH)

    @pl.when(core == 0)
    def _():
        halo[...] = jnp.zeros_like(halo)

    s_buf[...] = jnp.zeros_like(s_buf)
    h_buf[0:top, :] = jnp.zeros((top, chan), F32)
    pl.semaphore_wait(barrier, group_n - 1)

    half, place = me // batch_n, lax.rem(me, batch_n)
    x_copy.wait()

    def x_copies(off):
        seq = lax.rem(chip + off, batch_n)
        target = seq * cores + half
        dst = x_all.at[pl.ds(place * seq_dev, seq_dev)]

        def local():
            return pltpu.make_async_copy(x_in.at[seq], dst, x_recv.at[place])

        def remote():
            return pltpu.make_async_remote_copy(x_in.at[seq], dst, x_send.at[off], x_recv.at[place], device_id={"sp": target},
                                                device_id_type=pl.DeviceIdType.MESH)

        return target, local, remote

    for off in far_first:
        target, local, remote = x_copies(off)
        if off:
            remote().start()
        else:
            pl.when(target == me)(lambda: local().start())
            pl.when(target != me)(lambda: remote().start())
    for src in range(batch_n):
        dst = x_all.at[pl.ds(src * seq_dev, seq_dev)]
        pltpu.make_async_copy(dst, dst, x_recv.at[src]).wait()
    x = x_all[...]
    h_buf[top:, :] = x.astype(F32)
    u_buf[0, pad:, :] = x
    tail[0, starts[0]:starts[0] + sizes[0], :] = x[rows - sizes[0]:]

    def halo_copy(turn):
        part = pl.ds(turn * GROUP, GROUP)
        return pltpu.make_async_remote_copy(tail.at[part], halo.at[part], halo_send.at[turn], halo_recv.at[turn],
                                            device_id={"sp": jnp.minimum(me + 1, group_n - 1)}, device_id_type=pl.DeviceIdType.MESH)


    def dot(lhs, rhs):
        return jnp.dot(lhs, rhs, preferred_element_type=F32)

    def group_of_stacks(turn, carry):
        base = turn * GROUP
        for copy in weight_copies(turn):
            copy.wait()
        pl.when(core > 0)(lambda: halo_copy(turn).wait_recv())

        for layer in range(GROUP * cycle_len):
            part, pos = divmod(layer, cycle_len)
            at, dilation = (base + part, pos), 2**pos
            got = halo[base + part, starts[pos]:starts[pos] + sizes[pos], :]
            if dilation == 1:
                h_buf[0:top, :] = got[sizes[pos] - top:].astype(F32)
                past = h_buf[top - 1:top + rows - 1, :].astype(BF16)
            else:
                u_buf[pos, pad - sizes[pos]:pad, :] = got
                past = u_buf[pos, pad - dilation:pad - dilation + rows, :]
            taps = jnp.concatenate([u_buf[pos, pad:, :], past], axis=1)
            z = dot(taps, jnp.concatenate([w_cur[at], w_past[at]], axis=0))
            a = (jnp.tanh(z[:, :chan]) * (0.5 * jnp.tanh(0.5 * z[:, chan:]) + 0.5)).astype(BF16)
            out = dot(a, jnp.concatenate([w_res[at], w_skip[at]], axis=1))
            h = h_buf[top:, :] + out[:, :chan]
            h_buf[top:, :] = h
            s_buf[...] = s_buf[...] + out[:, chan:]
            u = h.astype(BF16)
            part, pos = divmod(layer + 1, cycle_len)
            u_buf[pos, pad:, :] = u
            tail[base + part, starts[pos]:starts[pos] + sizes[pos], :] = u[rows - sizes[pos]:]
        pl.when(core < cores - 1)(lambda: halo_copy(turn).start())
        return carry

    lax.fori_loop(0, stacks // GROUP, group_of_stacks, 0)

    part_rows = rows // group_n
    spread = [(off, sub) for off in far_first for sub in range(cores)]

    def out_target(off, sub):
        return lax.rem(chip + off, batch_n) * cores + sub

    def out_copies(off, sub):
        target = out_target(off, sub)
        dst = both_out.at[:, chip, core]

        def remote():
            return pltpu.make_async_remote_copy(stage.at[target], dst, out_send.at[off * cores + sub], out_recv.at[me],
                                                device_id={"sp": target}, device_id_type=pl.DeviceIdType.MESH)

        return target, remote

    def send(off, sub):
        target, remote = out_copies(off, sub)
        if off:
            remote().start()
        else:
            @pl.when(target == me)
            def _():
                both_out[:, chip, core] = stage[target]

            pl.when(target != me)(lambda: remote().start())

    for rank, (off, sub) in enumerate(spread):
        target = out_target(off, sub)
        stage[target, 1] = s_buf[pl.ds(target, part_rows, stride=group_n), :]
        stage[target, 0] = h_buf[pl.ds(top + target, part_rows, stride=group_n), :]
        if rank:
            send(*spread[rank - 1])
    send(*spread[-1])

    for off in range(batch_n):
        target, local, remote = x_copies(off)
        if off:
            remote().wait_send()
        else:
            pl.when(target != me)(lambda: remote().wait_send())

    def end_halo(turn, carry):
        halo_copy(turn).wait_send()
        return carry

    @pl.when(core < cores - 1)
    def _():
        lax.fori_loop(0, stacks // GROUP, end_halo, 0)

    for off, sub in spread:
        target, remote = out_copies(off, sub)
        if off:
            remote().wait_send()
        else:
            pl.when(target != me)(lambda: remote().wait_send())
    for src in range(group_n):
        dst = both_out.at[:, src // cores, src % cores]

        @pl.when(src != me)
        def _():
            pltpu.make_async_copy(dst, dst, out_recv.at[src]).wait()


def write_out(both, h_out, s_out, sems):
    copies = [pltpu.make_async_copy(both.at[kind], out, sems.at[kind]) for kind, out in enumerate((h_out, s_out))]
    for copy in copies:
        copy.start()
    for copy in copies:
        copy.wait()


def solution(mesh):
    group_n = mesh.shape["sp"]

    def local_stack(x, w_cur, w_past, w_res, w_skip):
        batch_n, seq_dev, chan = x.shape
        stacks, cycle_len = w_cur.shape[:2]
        rows = batch_n * seq_dev
        sizes, starts, halo_rows = halo_slots(cycle_len)
        pad, top = 2 ** (cycle_len - 1), 8
        turns = stacks // GROUP
        vmem, dma = pltpu.VMEM, pltpu.SemaphoreType.DMA
        cores, part_rows = group_n // batch_n, rows // group_n
        hbm, in_vmem = pl.BlockSpec(memory_space=pltpu.HBM), pl.BlockSpec(memory_space=vmem)
        both = pl.pallas_call(
            functools.partial(kernel, group_n),
            out_shape=vmem((2, batch_n, cores, part_rows, chan), F32),
            in_specs=[hbm] * 5,
            out_specs=in_vmem,
            scratch_shapes=[
                vmem(w_cur.shape, BF16), vmem(w_past.shape, BF16), vmem(w_res.shape, BF16), vmem(w_skip.shape, BF16),
                vmem((top + rows, chan), F32), vmem((rows, chan), F32), vmem((cycle_len, pad + rows, chan), BF16),
                vmem((stacks, halo_rows, chan), BF16), vmem((stacks + 1, halo_rows, chan), BF16),
                vmem(x.shape, BF16), vmem((rows, chan), BF16),
                vmem((group_n, 2, part_rows, chan), F32),
                dma((turns, 4)), dma, dma((batch_n,)), dma((batch_n,)), dma((turns,)), dma((turns,)), dma((group_n,)), dma((group_n,)),
            ],
            compiler_params=pltpu.CompilerParams(collective_id=0, has_side_effects=True, vmem_limit_bytes=50 * 2**20),
        )(pltpu.with_memory_space_constraint(x, pltpu.HBM), w_cur, w_past, w_res, w_skip)
        both = pltpu.with_memory_space_constraint(both, pltpu.VMEM)
        out = jax.ShapeDtypeStruct((batch_n, cores, part_rows, chan), F32)
        outs = pl.pallas_call(write_out, out_shape=[out, out], in_specs=[in_vmem], out_specs=[hbm] * 2, scratch_shapes=[dma((2,))])(both)
        return tuple(o.reshape(batch_n, 1, seq_dev, chan) for o in outs)

    return jax.shard_map(local_stack, mesh=mesh, in_specs=(P("dp", "sp", None), P(), P(), P(), P()),
                         out_specs=(P("dp", "sp", None, None), P("dp", "sp", None, None)), check_vma=False)
```

```python
import functools

import jax
import jax.numpy as jnp
from jax import lax
from jax.experimental import pallas as pl
from jax.experimental.pallas import tpu as pltpu
from jax.sharding import PartitionSpec as P

F32, BF16 = jnp.float32, jnp.bfloat16
GROUP = 2


def halo_slots(cycle_len):
    sizes = [max(16, 2**layer) for layer in range(cycle_len)]
    starts = [sum(sizes[:layer]) for layer in range(cycle_len)]
    return sizes, starts, sum(sizes)


def kernel(group_n, x_hbm, wc_hbm, wp_hbm, wr_hbm, ws_hbm, both_out, w_cur, w_past, w_res, w_skip, h_buf, s_buf, u_buf, halo, tail, x_in, x_all,
           stage, got_out, h_late, u_late, w_sem, x_sem, x_send, x_recv, halo_send, halo_recv, out_send, out_recv):
    batch_n, seq_dev, chan = x_in.shape
    stacks, cycle_len = w_cur.shape[:2]
    rows = batch_n * seq_dev
    cores = group_n // batch_n
    pad = u_buf.shape[1] - rows
    top = h_buf.shape[0] - rows
    sizes, starts, halo_rows = halo_slots(cycle_len)
    me = lax.axis_index("sp")
    chip, core = me // cores, lax.rem(me, cores)
    far_first = sorted(range(batch_n), key=lambda off: -min(off, batch_n - off))

    x_copy = pltpu.make_async_copy(x_hbm, x_in, x_sem)
    x_copy.start()
    pairs = ((wc_hbm, w_cur), (wp_hbm, w_past), (wr_hbm, w_res), (ws_hbm, w_skip))

    def weight_copies(turn):
        part = pl.ds(turn * GROUP, GROUP)
        return [pltpu.make_async_copy(src.at[part], dst.at[part], w_sem.at[turn, k]) for k, (src, dst) in enumerate(pairs)]

    for turn in range(stacks // GROUP):
        for copy in weight_copies(turn):
            copy.start(priority=1)

    barrier = pltpu.get_barrier_semaphore()
    for off in range(1, group_n):
        pl.semaphore_signal(barrier, inc=1, device_id={"sp": lax.rem(me + off, group_n)}, device_id_type=pl.DeviceIdType.MESH)

    @pl.when(core == 0)
    def _():
        halo[...] = jnp.zeros_like(halo)

    s_buf[...] = jnp.zeros_like(s_buf)
    h_buf[0:top, :] = jnp.zeros((top, chan), F32)
    pl.semaphore_wait(barrier, group_n - 1)

    half, place = me // batch_n, lax.rem(me, batch_n)
    x_copy.wait()

    def x_copies(off):
        seq = lax.rem(chip + off, batch_n)
        target = seq * cores + half
        dst = x_all.at[pl.ds(place * seq_dev, seq_dev)]

        def local():
            return pltpu.make_async_copy(x_in.at[seq], dst, x_recv.at[place])

        def remote():
            return pltpu.make_async_remote_copy(x_in.at[seq], dst, x_send.at[off], x_recv.at[place], device_id={"sp": target},
                                                device_id_type=pl.DeviceIdType.MESH)

        return target, local, remote

    for off in far_first:
        target, local, remote = x_copies(off)
        if off:
            remote().start()
        else:
            pl.when(target == me)(lambda: local().start())
            pl.when(target != me)(lambda: remote().start())
    for src in range(batch_n):
        dst = x_all.at[pl.ds(src * seq_dev, seq_dev)]
        pltpu.make_async_copy(dst, dst, x_recv.at[src]).wait()
    x = x_all[...]
    h_buf[top:, :] = x.astype(F32)
    u_buf[0, pad:, :] = x
    tail[0, starts[0]:starts[0] + sizes[0], :] = x[rows - sizes[0]:]

    def halo_copy(turn):
        part = pl.ds(turn * GROUP, GROUP)
        return pltpu.make_async_remote_copy(tail.at[part], halo.at[part], halo_send.at[turn], halo_recv.at[turn],
                                            device_id={"sp": jnp.minimum(me + 1, group_n - 1)}, device_id_type=pl.DeviceIdType.MESH)


    def dot(lhs, rhs):
        return jnp.dot(lhs, rhs, preferred_element_type=F32)

    late = sum(2**pos >= group_n for pos in range(cycle_len))

    def group_of_stacks(turn, layers):
        base = turn * GROUP
        for copy in weight_copies(turn):
            copy.wait()
        pl.when(core > 0)(lambda: halo_copy(turn).wait_recv())

        for layer in range(layers):
            part, pos = divmod(layer, cycle_len)
            at, dilation = (base + part, pos), 2**pos
            got = halo[base + part, starts[pos]:starts[pos] + sizes[pos], :]
            if dilation == 1:
                h_buf[0:top, :] = got[sizes[pos] - top:].astype(F32)
                past = h_buf[top - 1:top + rows - 1, :].astype(BF16)
            else:
                u_buf[pos, pad - sizes[pos]:pad, :] = got
                past = u_buf[pos, pad - dilation:pad - dilation + rows, :]
            taps = jnp.concatenate([u_buf[pos, pad:, :], past], axis=1)
            z = dot(taps, jnp.concatenate([w_cur[at], w_past[at]], axis=0))
            a = (jnp.tanh(z[:, :chan]) * (0.5 * jnp.tanh(0.5 * z[:, chan:]) + 0.5)).astype(BF16)
            out = dot(a, jnp.concatenate([w_res[at], w_skip[at]], axis=1))
            h = h_buf[top:, :] + out[:, :chan]
            h_buf[top:, :] = h
            s_buf[...] = s_buf[...] + out[:, chan:]
            u = h.astype(BF16)
            part, pos = divmod(layer + 1, cycle_len)
            u_buf[pos, pad:, :] = u
            tail[base + part, starts[pos]:starts[pos] + sizes[pos], :] = u[rows - sizes[pos]:]
        pl.when(core < cores - 1)(lambda: halo_copy(turn).start())

    def whole_turn(turn, carry):
        group_of_stacks(turn, GROUP * cycle_len)
        return carry

    turns = stacks // GROUP
    lax.fori_loop(0, turns - 1, whole_turn, 0)
    group_of_stacks(turns - 1, GROUP * cycle_len - late)

    part_rows = rows // group_n
    spread = [(off, sub) for off in far_first for sub in range(cores)]

    def out_target(off, sub):
        return lax.rem(chip + off, batch_n) * cores + sub

    def out_copy(kind, off, sub):
        target = out_target(off, sub)
        return pltpu.make_async_remote_copy(stage.at[kind, target], got_out.at[kind, chip, core], out_send.at[kind, off * cores + sub],
                                            out_recv.at[kind, me], device_id={"sp": target}, device_id_type=pl.DeviceIdType.MESH)

    def send(kind, off, sub):
        if off:
            out_copy(kind, off, sub).start()
        else:
            target = out_target(off, sub)

            @pl.when(target == me)
            def _():
                got_out[kind, chip, core] = stage[kind, target]

            pl.when(target != me)(lambda: out_copy(kind, off, sub).start())

    def receive(kind):
        for src in range(group_n):
            dst = got_out.at[kind, src // cores, src % cores]

            @pl.when(src != me)
            def _():
                pltpu.make_async_copy(dst, dst, out_recv.at[kind, src]).wait()

    for kind, buf, skipped in ((0, h_buf, top), (1, s_buf, 0)):
        for rank, (off, sub) in enumerate(spread):
            target = out_target(off, sub)
            stage[kind, target] = buf[pl.ds(skipped + target, part_rows, stride=group_n), :]
            if rank:
                send(kind, *spread[rank - 1])
        send(kind, *spread[-1])

    receive(0)
    pad_late = u_late.shape[1] - seq_dev
    h = got_out[0].reshape(batch_n, seq_dev, chan)
    h_late[:, 0:top, :] = jnp.zeros((batch_n, top, chan), F32)
    h_late[:, top:, :] = h
    u_late[:, 0:pad_late, :] = jnp.zeros((batch_n, pad_late, chan), BF16)
    u_late[:, pad_late:, :] = h.astype(BF16)
    for pos in range(cycle_len - late, cycle_len):
        at, shift = (stacks - 1, pos), 2**pos // group_n
        if shift == 1:
            past = h_late[:, top - 1:top + seq_dev - 1, :].astype(BF16)
        else:
            past = u_late[:, pad_late - shift:pad_late - shift + seq_dev, :]
        taps = jnp.concatenate([u_late[:, pad_late:, :], past], axis=2).reshape(rows, 2 * chan)
        z = dot(taps, jnp.concatenate([w_cur[at], w_past[at]], axis=0))
        a = (jnp.tanh(z[:, :chan]) * (0.5 * jnp.tanh(0.5 * z[:, chan:]) + 0.5)).astype(BF16)
        out = dot(a, jnp.concatenate([w_res[at], w_skip[at]], axis=1)).reshape(batch_n, seq_dev, 2 * chan)
        h = h_late[:, top:, :] + out[:, :, :chan]
        h_late[:, top:, :] = h
        u_late[:, pad_late:, :] = h.astype(BF16)
        more = out[:, :, chan:]
        if pos == cycle_len - late:
            both_out[1] = more
        else:
            both_out[1] = both_out[1] + more
    both_out[0] = h_late[:, top:, :]
    receive(1)
    both_out[1] = got_out[1].reshape(batch_n, seq_dev, chan) + both_out[1]

    for off in range(batch_n):
        target, local, remote = x_copies(off)
        if off:
            remote().wait_send()
        else:
            pl.when(target != me)(lambda: remote().wait_send())

    def end_halo(turn, carry):
        halo_copy(turn).wait_send()
        return carry

    @pl.when(core < cores - 1)
    def _():
        lax.fori_loop(0, stacks // GROUP, end_halo, 0)

    for kind in range(2):
        for off, sub in spread:
            if off:
                out_copy(kind, off, sub).wait_send()
            else:
                pl.when(out_target(off, sub) != me)(lambda: out_copy(kind, off, sub).wait_send())


def write_out(both, h_out, s_out, sems):
    copies = [pltpu.make_async_copy(both.at[kind], out, sems.at[kind]) for kind, out in enumerate((h_out, s_out))]
    for copy in copies:
        copy.start()
    for copy in copies:
        copy.wait()


def solution(mesh):
    group_n = mesh.shape["sp"]

    def local_stack(x, w_cur, w_past, w_res, w_skip):
        batch_n, seq_dev, chan = x.shape
        stacks, cycle_len = w_cur.shape[:2]
        rows = batch_n * seq_dev
        sizes, starts, halo_rows = halo_slots(cycle_len)
        pad, top = 2 ** (cycle_len - 1), 8
        pad_late = max(16, pad // group_n)
        turns = stacks // GROUP
        vmem, dma = pltpu.VMEM, pltpu.SemaphoreType.DMA
        cores, part_rows = group_n // batch_n, rows // group_n
        hbm, in_vmem = pl.BlockSpec(memory_space=pltpu.HBM), pl.BlockSpec(memory_space=vmem)
        both = pl.pallas_call(
            functools.partial(kernel, group_n),
            out_shape=vmem((2,) + x.shape, F32),
            in_specs=[hbm] * 5,
            out_specs=in_vmem,
            scratch_shapes=[
                vmem(w_cur.shape, BF16), vmem(w_past.shape, BF16), vmem(w_res.shape, BF16), vmem(w_skip.shape, BF16),
                vmem((top + rows, chan), F32), vmem((rows, chan), F32), vmem((cycle_len, pad + rows, chan), BF16),
                vmem((stacks, halo_rows, chan), BF16), vmem((stacks + 1, halo_rows, chan), BF16),
                vmem(x.shape, BF16), vmem((rows, chan), BF16),
                vmem((2, group_n, part_rows, chan), F32), vmem((2, batch_n, cores, part_rows, chan), F32),
                vmem((batch_n, top + seq_dev, chan), F32), vmem((batch_n, pad_late + seq_dev, chan), BF16),
                dma((turns, 4)), dma, dma((batch_n,)), dma((batch_n,)), dma((turns,)), dma((turns,)), dma((2, group_n)), dma((2, group_n)),
            ],
            compiler_params=pltpu.CompilerParams(collective_id=0, has_side_effects=True, vmem_limit_bytes=52 * 2**20),
        )(pltpu.with_memory_space_constraint(x, pltpu.HBM), w_cur, w_past, w_res, w_skip)
        both = pltpu.with_memory_space_constraint(both, pltpu.VMEM)
        out = jax.ShapeDtypeStruct(x.shape, F32)
        outs = pl.pallas_call(write_out, out_shape=[out, out], in_specs=[in_vmem], out_specs=[hbm] * 2, scratch_shapes=[dma((2,))])(both)
        return tuple(o.reshape(batch_n, 1, seq_dev, chan) for o in outs)

    return jax.shard_map(local_stack, mesh=mesh, in_specs=(P("dp", "sp", None), P(), P(), P(), P()),
                         out_specs=(P("dp", "sp", None, None), P("dp", "sp", None, None)), check_vma=False)
```

```python
import functools

import jax
import jax.numpy as jnp
from jax import lax
from jax.experimental import pallas as pl
from jax.experimental.pallas import tpu as pltpu
from jax.sharding import PartitionSpec as P

F32, BF16 = jnp.float32, jnp.bfloat16
GROUP = 2
UNROLL = 2


def halo_slots(cycle_len):
    sizes = [max(16, 2**layer) for layer in range(cycle_len)]
    starts = [sum(sizes[:layer]) for layer in range(cycle_len)]
    return sizes, starts, sum(sizes)


def kernel(group_n, x_hbm, wc_hbm, wp_hbm, wr_hbm, ws_hbm, both_out, w_cur, w_past, w_res, w_skip, h_buf, s_buf, u_buf, halo, tail, x_in, x_all,
           stage, got_out, h_late, u_late, w_sem, x_sem, x_send, x_recv, halo_send, halo_recv, out_send, out_recv):
    batch_n, seq_dev, chan = x_in.shape
    stacks, cycle_len = w_cur.shape[:2]
    rows = batch_n * seq_dev
    cores = group_n // batch_n
    pad = u_buf.shape[1] - rows
    top = h_buf.shape[0] - rows
    sizes, starts, halo_rows = halo_slots(cycle_len)
    me = lax.axis_index("sp")
    chip, core = me // cores, lax.rem(me, cores)
    far_first = sorted(range(batch_n), key=lambda off: -min(off, batch_n - off))

    x_copy = pltpu.make_async_copy(x_hbm, x_in, x_sem)
    x_copy.start()
    pairs = ((wc_hbm, w_cur), (wp_hbm, w_past), (wr_hbm, w_res), (ws_hbm, w_skip))

    def weight_copies(turn):
        part = pl.ds(turn * GROUP, GROUP)
        return [pltpu.make_async_copy(src.at[part], dst.at[part], w_sem.at[turn, k]) for k, (src, dst) in enumerate(pairs)]

    for turn in range(stacks // GROUP):
        for copy in weight_copies(turn):
            copy.start(priority=1)

    barrier = pltpu.get_barrier_semaphore()
    for off in range(1, group_n):
        pl.semaphore_signal(barrier, inc=1, device_id={"sp": lax.rem(me + off, group_n)}, device_id_type=pl.DeviceIdType.MESH)

    @pl.when(core == 0)
    def _():
        halo[...] = jnp.zeros_like(halo)

    s_buf[...] = jnp.zeros_like(s_buf)
    h_buf[0:top, :] = jnp.zeros((top, chan), F32)
    pl.semaphore_wait(barrier, group_n - 1)

    half, place = me // batch_n, lax.rem(me, batch_n)
    x_copy.wait()

    def x_copies(off):
        seq = lax.rem(chip + off, batch_n)
        target = seq * cores + half
        dst = x_all.at[pl.ds(place * seq_dev, seq_dev)]

        def local():
            return pltpu.make_async_copy(x_in.at[seq], dst, x_recv.at[place])

        def remote():
            return pltpu.make_async_remote_copy(x_in.at[seq], dst, x_send.at[off], x_recv.at[place], device_id={"sp": target},
                                                device_id_type=pl.DeviceIdType.MESH)

        return target, local, remote

    for off in far_first:
        target, local, remote = x_copies(off)
        if off:
            remote().start()
        else:
            pl.when(target == me)(lambda: local().start())
            pl.when(target != me)(lambda: remote().start())
    for src in range(batch_n):
        dst = x_all.at[pl.ds(src * seq_dev, seq_dev)]
        pltpu.make_async_copy(dst, dst, x_recv.at[src]).wait()
    x = x_all[...]
    h_buf[top:, :] = x.astype(F32)
    u_buf[0, pad:, :] = x
    tail[0, starts[0]:starts[0] + sizes[0], :] = x[rows - sizes[0]:]

    def halo_copy(turn):
        part = pl.ds(turn * GROUP, GROUP)
        return pltpu.make_async_remote_copy(tail.at[part], halo.at[part], halo_send.at[turn], halo_recv.at[turn],
                                            device_id={"sp": jnp.minimum(me + 1, group_n - 1)}, device_id_type=pl.DeviceIdType.MESH)


    def dot(lhs, rhs):
        return jnp.dot(lhs, rhs, preferred_element_type=F32)

    late = sum(2**pos >= group_n for pos in range(cycle_len))

    def group_of_stacks(turn, layers):
        base = turn * GROUP
        for copy in weight_copies(turn):
            copy.wait()
        pl.when(core > 0)(lambda: halo_copy(turn).wait_recv())

        for layer in range(layers):
            part, pos = divmod(layer, cycle_len)
            at, dilation = (base + part, pos), 2**pos
            got = halo[base + part, starts[pos]:starts[pos] + sizes[pos], :]
            if dilation == 1:
                h_buf[0:top, :] = got[sizes[pos] - top:].astype(F32)
                past = h_buf[top - 1:top + rows - 1, :].astype(BF16)
            else:
                u_buf[pos, pad - sizes[pos]:pad, :] = got
                past = u_buf[pos, pad - dilation:pad - dilation + rows, :]
            taps = jnp.concatenate([u_buf[pos, pad:, :], past], axis=1)
            z = dot(taps, jnp.concatenate([w_cur[at], w_past[at]], axis=0))
            a = (jnp.tanh(z[:, :chan]) * (0.5 * jnp.tanh(0.5 * z[:, chan:]) + 0.5)).astype(BF16)
            out = dot(a, jnp.concatenate([w_res[at], w_skip[at]], axis=1))
            h = h_buf[top:, :] + out[:, :chan]
            h_buf[top:, :] = h
            s_buf[...] = s_buf[...] + out[:, chan:]
            u = h.astype(BF16)
            part, pos = divmod(layer + 1, cycle_len)
            u_buf[pos, pad:, :] = u
            tail[base + part, starts[pos]:starts[pos] + sizes[pos], :] = u[rows - sizes[pos]:]
        pl.when(core < cores - 1)(lambda: halo_copy(turn).start())

    turns = stacks // GROUP

    def body(trip, carry):
        for k in range(UNROLL):
            group_of_stacks(trip * UNROLL + k, GROUP * cycle_len)
        return carry

    trips = (turns - 1) // UNROLL
    lax.fori_loop(0, trips, body, 0)
    for turn in range(trips * UNROLL, turns):
        group_of_stacks(turn, GROUP * cycle_len - (late if turn == turns - 1 else 0))

    part_rows = rows // group_n
    spread = [(off, sub) for off in far_first for sub in range(cores)]

    def out_target(off, sub):
        return lax.rem(chip + off, batch_n) * cores + sub

    def out_copy(kind, off, sub):
        target = out_target(off, sub)
        return pltpu.make_async_remote_copy(stage.at[kind, target], got_out.at[kind, chip, core], out_send.at[kind, off * cores + sub],
                                            out_recv.at[kind, me], device_id={"sp": target}, device_id_type=pl.DeviceIdType.MESH)

    def send(kind, off, sub):
        if off:
            out_copy(kind, off, sub).start()
        else:
            target = out_target(off, sub)

            @pl.when(target == me)
            def _():
                got_out[kind, chip, core] = stage[kind, target]

            pl.when(target != me)(lambda: out_copy(kind, off, sub).start())

    def receive(kind):
        for src in range(group_n):
            dst = got_out.at[kind, src // cores, src % cores]

            @pl.when(src != me)
            def _():
                pltpu.make_async_copy(dst, dst, out_recv.at[kind, src]).wait()

    for kind, buf, skipped in ((0, h_buf, top), (1, s_buf, 0)):
        for rank, (off, sub) in enumerate(spread):
            target = out_target(off, sub)
            stage[kind, target] = buf[pl.ds(skipped + target, part_rows, stride=group_n), :]
            if rank:
                send(kind, *spread[rank - 1])
        send(kind, *spread[-1])

    receive(0)
    pad_late = u_late.shape[1] - seq_dev
    h = got_out[0].reshape(batch_n, seq_dev, chan)
    h_late[:, 0:top, :] = jnp.zeros((batch_n, top, chan), F32)
    h_late[:, top:, :] = h
    u_late[:, 0:pad_late, :] = jnp.zeros((batch_n, pad_late, chan), BF16)
    u_late[:, pad_late:, :] = h.astype(BF16)
    for pos in range(cycle_len - late, cycle_len):
        at, shift = (stacks - 1, pos), 2**pos // group_n
        if shift == 1:
            past = h_late[:, top - 1:top + seq_dev - 1, :].astype(BF16)
        else:
            past = u_late[:, pad_late - shift:pad_late - shift + seq_dev, :]
        taps = jnp.concatenate([u_late[:, pad_late:, :], past], axis=2).reshape(rows, 2 * chan)
        z = dot(taps, jnp.concatenate([w_cur[at], w_past[at]], axis=0))
        a = (jnp.tanh(z[:, :chan]) * (0.5 * jnp.tanh(0.5 * z[:, chan:]) + 0.5)).astype(BF16)
        out = dot(a, jnp.concatenate([w_res[at], w_skip[at]], axis=1)).reshape(batch_n, seq_dev, 2 * chan)
        h = h_late[:, top:, :] + out[:, :, :chan]
        h_late[:, top:, :] = h
        u_late[:, pad_late:, :] = h.astype(BF16)
        more = out[:, :, chan:]
        if pos == cycle_len - late:
            both_out[1] = more
        else:
            both_out[1] = both_out[1] + more
    both_out[0] = h_late[:, top:, :]
    receive(1)
    both_out[1] = got_out[1].reshape(batch_n, seq_dev, chan) + both_out[1]

    for off in range(batch_n):
        target, local, remote = x_copies(off)
        if off:
            remote().wait_send()
        else:
            pl.when(target != me)(lambda: remote().wait_send())

    def end_halo(turn, carry):
        halo_copy(turn).wait_send()
        return carry

    @pl.when(core < cores - 1)
    def _():
        lax.fori_loop(0, stacks // GROUP, end_halo, 0)

    for kind in range(2):
        for off, sub in spread:
            if off:
                out_copy(kind, off, sub).wait_send()
            else:
                pl.when(out_target(off, sub) != me)(lambda: out_copy(kind, off, sub).wait_send())


def write_out(both, h_out, s_out, sems):
    copies = [pltpu.make_async_copy(both.at[kind], out, sems.at[kind]) for kind, out in enumerate((h_out, s_out))]
    for copy in copies:
        copy.start()
    for copy in copies:
        copy.wait()


def solution(mesh):
    group_n = mesh.shape["sp"]

    def local_stack(x, w_cur, w_past, w_res, w_skip):
        batch_n, seq_dev, chan = x.shape
        stacks, cycle_len = w_cur.shape[:2]
        rows = batch_n * seq_dev
        sizes, starts, halo_rows = halo_slots(cycle_len)
        pad, top = 2 ** (cycle_len - 1), 8
        pad_late = max(16, pad // group_n)
        turns = stacks // GROUP
        vmem, dma = pltpu.VMEM, pltpu.SemaphoreType.DMA
        cores, part_rows = group_n // batch_n, rows // group_n
        hbm, in_vmem = pl.BlockSpec(memory_space=pltpu.HBM), pl.BlockSpec(memory_space=vmem)
        both = pl.pallas_call(
            functools.partial(kernel, group_n),
            out_shape=vmem((2,) + x.shape, F32),
            in_specs=[hbm] * 5,
            out_specs=in_vmem,
            scratch_shapes=[
                vmem(w_cur.shape, BF16), vmem(w_past.shape, BF16), vmem(w_res.shape, BF16), vmem(w_skip.shape, BF16),
                vmem((top + rows, chan), F32), vmem((rows, chan), F32), vmem((cycle_len, pad + rows, chan), BF16),
                vmem((stacks, halo_rows, chan), BF16), vmem((stacks + 1, halo_rows, chan), BF16),
                vmem(x.shape, BF16), vmem((rows, chan), BF16),
                vmem((2, group_n, part_rows, chan), F32), vmem((2, batch_n, cores, part_rows, chan), F32),
                vmem((batch_n, top + seq_dev, chan), F32), vmem((batch_n, pad_late + seq_dev, chan), BF16),
                dma((turns, 4)), dma, dma((batch_n,)), dma((batch_n,)), dma((turns,)), dma((turns,)), dma((2, group_n)), dma((2, group_n)),
            ],
            compiler_params=pltpu.CompilerParams(collective_id=0, has_side_effects=True, vmem_limit_bytes=52 * 2**20),
        )(pltpu.with_memory_space_constraint(x, pltpu.HBM), w_cur, w_past, w_res, w_skip)
        both = pltpu.with_memory_space_constraint(both, pltpu.VMEM)
        out = jax.ShapeDtypeStruct(x.shape, F32)
        outs = pl.pallas_call(write_out, out_shape=[out, out], in_specs=[in_vmem], out_specs=[hbm] * 2, scratch_shapes=[dma((2,))])(both)
        return tuple(o.reshape(batch_n, 1, seq_dev, chan) for o in outs)

    return jax.shard_map(local_stack, mesh=mesh, in_specs=(P("dp", "sp", None), P(), P(), P(), P()),
                         out_specs=(P("dp", "sp", None, None), P("dp", "sp", None, None)), check_vma=False)
```

```python
import functools

import jax
import jax.numpy as jnp
from jax import lax
from jax.experimental import pallas as pl
from jax.experimental.pallas import tpu as pltpu
from jax.sharding import PartitionSpec as P

F32, BF16 = jnp.float32, jnp.bfloat16
GROUP = 2
UNROLL = 2


def halo_slots(cycle_len):
    sizes = [max(16, 2**layer) for layer in range(cycle_len)]
    starts = [sum(sizes[:layer]) for layer in range(cycle_len)]
    return sizes, starts, sum(sizes)


def kernel(group_n, x_hbm, wc_hbm, wp_hbm, wr_hbm, ws_hbm, both_out, w_cur, w_past, w_res, w_skip, h_buf, s_buf, u_buf, halo, tail, x_in, x_all,
           stage, got_out, h_late, u_late, w_sem, x_sem, x_send, x_recv, halo_send, halo_recv, out_send, out_recv):
    batch_n, seq_dev, chan = x_in.shape
    stacks, cycle_len = w_cur.shape[:2]
    rows = batch_n * seq_dev
    cores = group_n // batch_n
    pad = u_buf.shape[1] - rows
    top = h_buf.shape[0] - rows
    sizes, starts, halo_rows = halo_slots(cycle_len)
    me = lax.axis_index("sp")
    chip, core = me // cores, lax.rem(me, cores)
    far_first = sorted(range(batch_n), key=lambda off: -min(off, batch_n - off))

    x_copy = pltpu.make_async_copy(x_hbm, x_in, x_sem)
    x_copy.start()
    pairs = ((wc_hbm, w_cur), (wp_hbm, w_past), (wr_hbm, w_res), (ws_hbm, w_skip))

    def weight_copies(turn):
        part = pl.ds(turn * GROUP, GROUP)
        return [pltpu.make_async_copy(src.at[part], dst.at[part], w_sem.at[turn, k]) for k, (src, dst) in enumerate(pairs)]

    for turn in range(stacks // GROUP):
        for copy in weight_copies(turn):
            copy.start(priority=1)

    barrier = pltpu.get_barrier_semaphore()
    for off in range(1, group_n):
        pl.semaphore_signal(barrier, inc=1, device_id={"sp": lax.rem(me + off, group_n)}, device_id_type=pl.DeviceIdType.MESH)

    @pl.when(core == 0)
    def _():
        halo[...] = jnp.zeros_like(halo)

    s_buf[...] = jnp.zeros_like(s_buf)
    h_buf[0:top, :] = jnp.zeros((top, chan), F32)
    pl.semaphore_wait(barrier, group_n - 1)

    half, place = me // batch_n, lax.rem(me, batch_n)
    x_copy.wait()

    def x_copies(off):
        seq = lax.rem(chip + off, batch_n)
        target = seq * cores + half
        dst = x_all.at[pl.ds(place * seq_dev, seq_dev)]

        def local():
            return pltpu.make_async_copy(x_in.at[seq], dst, x_recv.at[place])

        def remote():
            return pltpu.make_async_remote_copy(x_in.at[seq], dst, x_send.at[off], x_recv.at[place], device_id={"sp": target},
                                                device_id_type=pl.DeviceIdType.MESH)

        return target, local, remote

    for off in far_first:
        target, local, remote = x_copies(off)
        if off:
            remote().start()
        else:
            pl.when(target == me)(lambda: local().start())
            pl.when(target != me)(lambda: remote().start())
    for src in range(batch_n):
        dst = x_all.at[pl.ds(src * seq_dev, seq_dev)]
        pltpu.make_async_copy(dst, dst, x_recv.at[src]).wait()
    x = x_all[...]
    h_buf[top:, :] = x.astype(F32)
    u_buf[0, pad:, :] = x
    tail[0, starts[0]:starts[0] + sizes[0], :] = x[rows - sizes[0]:]

    def halo_copy(turn):
        part = pl.ds(turn * GROUP, GROUP)
        return pltpu.make_async_remote_copy(tail.at[part], halo.at[part], halo_send.at[turn], halo_recv.at[turn],
                                            device_id={"sp": jnp.minimum(me + 1, group_n - 1)}, device_id_type=pl.DeviceIdType.MESH)


    def dot(lhs, rhs):
        return jnp.dot(lhs, rhs, preferred_element_type=F32)

    late = sum(2**pos >= group_n for pos in range(cycle_len))

    def group_of_stacks(turn, layers):
        base = turn * GROUP
        for copy in weight_copies(turn):
            copy.wait()
        pl.when(core > 0)(lambda: halo_copy(turn).wait_recv())

        for layer in range(layers):
            part, pos = divmod(layer, cycle_len)
            at, dilation = (base + part, pos), 2**pos
            got = halo[base + part, starts[pos]:starts[pos] + sizes[pos], :]
            if dilation == 1:
                h_buf[0:top, :] = got[sizes[pos] - top:].astype(F32)
                past = h_buf[top - 1:top + rows - 1, :].astype(BF16)
            else:
                u_buf[pos, pad - sizes[pos]:pad, :] = got
                past = u_buf[pos, pad - dilation:pad - dilation + rows, :]
            taps = jnp.concatenate([u_buf[pos, pad:, :], past], axis=1)
            z = dot(taps, jnp.concatenate([w_cur[at], w_past[at]], axis=0))
            a = (jnp.tanh(z[:, :chan]) * (0.5 * jnp.tanh(0.5 * z[:, chan:]) + 0.5)).astype(BF16)
            out = dot(a, jnp.concatenate([w_res[at], w_skip[at]], axis=1))
            h = h_buf[top:, :] + out[:, :chan]
            h_buf[top:, :] = h
            s_buf[...] = s_buf[...] + out[:, chan:]
            u = h.astype(BF16)
            part, pos = divmod(layer + 1, cycle_len)
            u_buf[pos, pad:, :] = u
            tail[base + part, starts[pos]:starts[pos] + sizes[pos], :] = u[rows - sizes[pos]:]
        pl.when(core < cores - 1)(lambda: halo_copy(turn).start())

    turns = stacks // GROUP

    def body(trip, carry):
        for k in range(UNROLL):
            group_of_stacks(trip * UNROLL + k, GROUP * cycle_len)
        return carry

    trips = (turns - 1) // UNROLL
    lax.fori_loop(0, trips, body, 0)
    for turn in range(trips * UNROLL, turns):
        group_of_stacks(turn, GROUP * cycle_len - (late if turn == turns - 1 else 0))

    part_rows = rows // group_n
    spread = [(off, sub) for off in far_first for sub in range(cores)]

    def out_target(off, sub):
        return lax.rem(chip + off, batch_n) * cores + sub

    def out_copy(kind, off, sub):
        target = out_target(off, sub)
        return pltpu.make_async_remote_copy(stage.at[kind, target], got_out.at[kind, chip, core], out_send.at[kind, off * cores + sub],
                                            out_recv.at[kind, me], device_id={"sp": target}, device_id_type=pl.DeviceIdType.MESH)

    def send(kind, off, sub):
        if off:
            out_copy(kind, off, sub).start()
        else:
            target = out_target(off, sub)

            @pl.when(target == me)
            def _():
                got_out[kind, chip, core] = stage[kind, target]

            pl.when(target != me)(lambda: out_copy(kind, off, sub).start())

    def receive(kind):
        for src in range(group_n):
            dst = got_out.at[kind, src // cores, src % cores]

            @pl.when(src != me)
            def _():
                pltpu.make_async_copy(dst, dst, out_recv.at[kind, src]).wait()

    for kind, buf, skipped in ((0, h_buf, top), (1, s_buf, 0)):
        for rank, (off, sub) in enumerate(spread):
            target = out_target(off, sub)
            stage[kind, target] = buf[pl.ds(skipped + target, part_rows, stride=group_n), :]
            if rank:
                send(kind, *spread[rank - 1])
        send(kind, *spread[-1])

    receive(0)
    pad_late = u_late.shape[1] - seq_dev
    h = got_out[0].reshape(batch_n, seq_dev, chan)
    h_late[:, 0:top, :] = jnp.zeros((batch_n, top, chan), F32)
    h_late[:, top:, :] = h
    u_late[:, 0:pad_late, :] = jnp.zeros((batch_n, pad_late, chan), BF16)
    u_late[:, pad_late:, :] = h.astype(BF16)
    for pos in range(cycle_len - late, cycle_len):
        at, shift = (stacks - 1, pos), 2**pos // group_n
        if shift == 1:
            past = h_late[:, top - 1:top + seq_dev - 1, :].astype(BF16)
        else:
            past = u_late[:, pad_late - shift:pad_late - shift + seq_dev, :]
        taps = jnp.concatenate([u_late[:, pad_late:, :], past], axis=2).reshape(rows, 2 * chan)
        z = dot(taps, jnp.concatenate([w_cur[at], w_past[at]], axis=0))
        a = (jnp.tanh(z[:, :chan]) * (0.5 * jnp.tanh(0.5 * z[:, chan:]) + 0.5)).astype(BF16)
        out = dot(a, jnp.concatenate([w_res[at], w_skip[at]], axis=1)).reshape(batch_n, seq_dev, 2 * chan)
        h = h_late[:, top:, :] + out[:, :, :chan]
        h_late[:, top:, :] = h
        u_late[:, pad_late:, :] = h.astype(BF16)
        more = out[:, :, chan:]
        if pos == cycle_len - late:
            both_out[1] = more
        else:
            both_out[1] = both_out[1] + more
    both_out[0] = h_late[:, top:, :]
    for off in range(batch_n):
        target, local, remote = x_copies(off)
        if off:
            remote().wait_send()
        else:
            pl.when(target != me)(lambda: remote().wait_send())

    def end_halo(turn, carry):
        halo_copy(turn).wait_send()
        return carry

    @pl.when(core < cores - 1)
    def _():
        lax.fori_loop(0, stacks // GROUP, end_halo, 0)

    for kind in range(2):
        for off, sub in spread:
            if off:
                out_copy(kind, off, sub).wait_send()
            else:
                pl.when(out_target(off, sub) != me)(lambda: out_copy(kind, off, sub).wait_send())

    receive(1)
    both_out[1] = got_out[1].reshape(batch_n, seq_dev, chan) + both_out[1]


def write_out(both, h_out, s_out, sems):
    copies = [pltpu.make_async_copy(both.at[kind], out, sems.at[kind]) for kind, out in enumerate((h_out, s_out))]
    for copy in copies:
        copy.start()
    for copy in copies:
        copy.wait()


def solution(mesh):
    group_n = mesh.shape["sp"]

    def local_stack(x, w_cur, w_past, w_res, w_skip):
        batch_n, seq_dev, chan = x.shape
        stacks, cycle_len = w_cur.shape[:2]
        rows = batch_n * seq_dev
        sizes, starts, halo_rows = halo_slots(cycle_len)
        pad, top = 2 ** (cycle_len - 1), 8
        pad_late = max(16, pad // group_n)
        turns = stacks // GROUP
        vmem, dma = pltpu.VMEM, pltpu.SemaphoreType.DMA
        cores, part_rows = group_n // batch_n, rows // group_n
        hbm, in_vmem = pl.BlockSpec(memory_space=pltpu.HBM), pl.BlockSpec(memory_space=vmem)
        both = pl.pallas_call(
            functools.partial(kernel, group_n),
            out_shape=vmem((2,) + x.shape, F32),
            in_specs=[hbm] * 5,
            out_specs=in_vmem,
            scratch_shapes=[
                vmem(w_cur.shape, BF16), vmem(w_past.shape, BF16), vmem(w_res.shape, BF16), vmem(w_skip.shape, BF16),
                vmem((top + rows, chan), F32), vmem((rows, chan), F32), vmem((cycle_len, pad + rows, chan), BF16),
                vmem((stacks, halo_rows, chan), BF16), vmem((stacks + 1, halo_rows, chan), BF16),
                vmem(x.shape, BF16), vmem((rows, chan), BF16),
                vmem((2, group_n, part_rows, chan), F32), vmem((2, batch_n, cores, part_rows, chan), F32),
                vmem((batch_n, top + seq_dev, chan), F32), vmem((batch_n, pad_late + seq_dev, chan), BF16),
                dma((turns, 4)), dma, dma((batch_n,)), dma((batch_n,)), dma((turns,)), dma((turns,)), dma((2, group_n)), dma((2, group_n)),
            ],
            compiler_params=pltpu.CompilerParams(collective_id=0, has_side_effects=True, vmem_limit_bytes=52 * 2**20),
        )(pltpu.with_memory_space_constraint(x, pltpu.HBM), w_cur, w_past, w_res, w_skip)
        both = pltpu.with_memory_space_constraint(both, pltpu.VMEM)
        out = jax.ShapeDtypeStruct(x.shape, F32)
        outs = pl.pallas_call(write_out, out_shape=[out, out], in_specs=[in_vmem], out_specs=[hbm] * 2, scratch_shapes=[dma((2,))])(both)
        return tuple(o.reshape(batch_n, 1, seq_dev, chan) for o in outs)

    return jax.shard_map(local_stack, mesh=mesh, in_specs=(P("dp", "sp", None), P(), P(), P(), P()),
                         out_specs=(P("dp", "sp", None, None), P("dp", "sp", None, None)), check_vma=False)
```
